32 devices in a mesh: cell: 4 (over z), tm: 8 (over y, x, core).
Axes of the slice: x: 2, y: 2, z: 4, core: 2. Of those that a mesh axis runs over, the one named last changes fastest.
Arguments:
- solution: float32 [8192], P(('cell', 'tm')), may hold values from -6 to 6
- residual: float32 [8192], P(('cell', 'tm')), may hold values from -8 to 8
- direction: float32 [8192], P(('cell', 'tm')), may hold values from -8 to 8
- noise_var: float32 [8192], P(('cell', 'tm')), may hold values from 0.5 to 2
- footprints: bfloat16 [65536, 128], P(('cell', 'tm')), may hold values from -0.5 to 0.5
- tile_owner: int32 [65536, 1], P(('cell', 'tm')), may hold values from 0 to 31; in each aligned block of 2048 rows (0 to 2047, 2048 to 4095, ...) at most 128 rows name the same one
- tile_block: int32 [65536], P(('cell', 'tm')), may hold values from 0 to 17
- tile_step: int32 [65536], P(('cell', 'tm')), may hold values from 0 to 255
- tile_obs: int32 [65536], P(('cell', 'tm')), may hold values from 0 to 255
- cell_cov: bfloat16 [9216, 9216], P('cell'), may hold values from -2 to 7, as said below
- time_cov: bfloat16 [2048, 2048], P('tm'), may hold values from -2 to 7, as said below
Outputs:
- new_solution: float32 [8192], P(('cell', 'tm'))
- new_residual: float32 [8192], P(('cell', 'tm'))
- new_direction: float32 [8192], P(('cell', 'tm'))
The draws below stay inside these ranges and needn't reach their ends.
Inputs may be any that keep to these rules, and one draw needn't show every extreme that they name: `tile_owner`: among the 2048 tiles of one device, no owner is named by more than 128 of them. `cell_cov`: symmetric positive definite. `time_cov`: symmetric positive definite.
All inputs are finite; a program needn't handle non-finite values.
Results may differ from the reference program's by a relative error of at most 0.0021.
Values may be sent and summed in bfloat16 or wider, within the bound.
No kernel may reach another device: no remote copies, remote signals or barrier semaphores. Data moves between devices by JAX's collectives and lax.ppermute only.
A program may use at most 128 MiB of HBM per device.

```python
import math
import jax
import jax.numpy as jnp
import numpy as np

BLK = 128
NC = 9216
NT = 2048
TPO = 8
OBS_DEV = 256
TILE_DEV = 2048
MOST = 128
CB_DEV = 18
T_DEV = 256
NOBS = 8192
NTILES = 65536
N_CELL = 4
N_TM = 8


def rising_vector(key, salt):
    key = jax.random.fold_in(key, salt)
    devices = NOBS // OBS_DEV
    position = (jnp.arange(NOBS) // OBS_DEV).astype(jnp.float32) / max(devices - 1, 1)
    values = jax.random.normal(key, (NOBS,), jnp.float32) * (0.6 + 1.2 * position)
    return jnp.clip(values, -8.0, 8.0)


def cov_matrix(key, order, salt):
    key = jax.random.fold_in(key, salt)
    key_scale, key_noise = jax.random.split(key)
    length = max(order / 4.0, 4.0)
    smooth_weight = 6.0 / math.sqrt(length + 4.0)
    ratio = math.exp(-2.0 / length)
    row_energy = 2.0 * ratio / (1.0 - ratio)
    noise_scale = 0.4 / math.sqrt(row_energy)
    scales = jnp.exp(jax.random.uniform(key_scale, (order,), jnp.float32, math.log(0.8), math.log(1.25)))
    position = jnp.arange(order).astype(jnp.float32)
    distance = jnp.abs(position[:, None] - position[None, :])
    decay = jnp.exp(-distance / length)
    identity = jnp.eye(order, dtype=jnp.float32)
    raw = jax.random.normal(key_noise, (order, order), jnp.float32)
    symmetric = jnp.clip((raw + raw.T) * 0.7071, -4.0, 4.0) * (1.0 - identity)
    core = 1.5 * identity + smooth_weight * decay + noise_scale * decay * symmetric
    return (scales[:, None] * core * scales[None, :]).astype(jnp.bfloat16)


def draw_residual(key, part):
    return rising_vector(key, 11)


def draw_direction(key, part):
    return rising_vector(key, 23)


def draw_cell_cov(key, part):
    return cov_matrix(key, NC, 37)


def draw_time_cov(key, part):
    return cov_matrix(key, NT, 41)


def plant(entries, key, low, largest):
    longest = entries.shape.index(max(entries.shape))
    spots = []
    for shift in (0, 1):
        where = [jax.random.randint(jax.random.fold_in(key, axis), (), 0, length) for axis, length in enumerate(entries.shape)]
        where[longest] = (where[longest] + shift) % entries.shape[longest]
        spots.append(tuple(where))
    return entries.at[spots[0]].set(low).at[spots[1]].set(largest)


def level_of(stream_key, shape, shards, least, largest):
    gain = 1.0
    for axis_at, blocks in shards:
        draws = jax.random.uniform(jax.random.fold_in(jax.random.fold_in(stream_key, 6), axis_at), (blocks,), jnp.float32, least / len(shards), largest / len(shards))
        gain = gain * jnp.repeat(jnp.exp(draws), shape[axis_at] // blocks).reshape((-1,) + (1,) * (len(shape) - 1 - axis_at))
    return gain


def deal_out(own_key, own, number, rows, amount, top, limit, lean):
    ranking = jax.random.permutation(own_key, amount)
    packed, ordinary = load_shares(amount, rows * top, limit, lean, True), load_shares(amount, rows * top, limit, lean, False)
    places = jnp.arange(amount)

    def named(sizes, rotation):
        used = int((sizes > 0).sum())
        fixed = max(1, used // 4)
        passed = fixed + (places - fixed + rotation * (used - fixed)) % max(1, amount - fixed)
        return jnp.zeros((amount,), jnp.int32).at[ranking[jnp.where(places < fixed, places, passed)]].set(jnp.asarray(sizes, jnp.int32))

    sizes = jnp.where(number % 4 == 0, named(packed, number // 4), named(ordinary, number - number // 4 - 1))
    mixed = jax.random.permutation(jax.random.fold_in(own, 3), amount)
    giver, sink = mixed[0:amount // 2 * 2:2], mixed[1:amount // 2 * 2:2]
    slack = jnp.minimum(sizes[giver] - 1, limit - sizes[sink]) // 2
    slack = jnp.where((giver == ranking[0]) | (sink == ranking[0]) | (sizes[sink] == 0), 0, jnp.maximum(slack, 0))
    passed = jax.random.randint(jax.random.fold_in(own, 4), (amount // 2,), 0, 1 << 20) % (slack + 1)
    sizes = sizes.at[giver].add(-passed).at[sink].add(passed)
    labels = jnp.searchsorted(jnp.cumsum(sizes), jnp.arange(rows * top), side="right").astype(jnp.int32)
    listing = labels.reshape(top, rows).T
    listing = listing[jax.random.permutation(jax.random.fold_in(own, 1), rows)]
    rotation = jax.random.randint(jax.random.fold_in(own, 2), (rows, 1), 0, top)
    return jnp.take_along_axis(listing, (jnp.arange(top)[None, :] + rotation) % top, axis=1)


def load_shares(amount, total, most, lean, full):
    loads = [(1 << 20) // math.isqrt(rank ** lean) + 1 for rank in range(1, amount + 1)]
    largest = most if full else min(most, max(-(-total // amount), total * loads[0] // sum(loads)))
    least = 1 if total - largest >= amount - 1 else 0
    counts, rest = [largest] + [least] * (amount - 1), total - largest - least * (amount - 1)
    while rest > 0:
        free = [i for i in range(1, amount) if counts[i] < largest] or [i for i in range(1, amount) if counts[i] < most]
        whole, left = sum([loads[i] for i in free]), rest
        for i in free:
            addition = min(most - counts[i], max(1, left * loads[i] // whole), rest)
            counts[i] = counts[i] + addition
            rest = rest - addition
    return np.array(counts)


def noise(rng, shape, deviation, most, cuts=(), kind=jnp.bfloat16):
    gain = level_of(rng, shape, cuts, -0.22, 0.18) if cuts else 1.0
    array = jax.random.normal(rng, shape, jnp.float32) * deviation * gain
    return jnp.minimum(jnp.maximum(array, -most), most).astype(kind)


def setup_inputs(seed: int = 0) -> dict:
    streams_of = jax.random.split(jax.random.key(seed), 12)
    solution = noise(streams_of[0], (NOBS,), 1.0, 6.0, ((0, 32),), jnp.float32)
    residual = draw_residual(jax.random.fold_in(streams_of[11], 71), 0)
    direction = draw_direction(jax.random.fold_in(streams_of[11], 71), 0)
    noise_var = jnp.clip(jnp.exp(math.log(2.0) - 1.3862944 * jax.random.uniform(streams_of[3], (NOBS,), jnp.float32) ** level_of(streams_of[3], (NOBS,), ((0, 32),), -0.2, 0.2)), 0.5, 2.0)
    footprints = noise(streams_of[4], (NTILES, BLK), ((BLK * TPO) ** -0.5), 0.5, ((0, 32),))
    tile_owner_keys = jax.random.split(jax.random.fold_in(streams_of[5], 1), NTILES // TILE_DEV)
    tile_owner_turns = jax.random.permutation(jax.random.fold_in(streams_of[5], 3), NTILES // TILE_DEV)
    tile_owner = jax.vmap(lambda own, number: deal_out(jax.random.fold_in(streams_of[5], 2), own, number, TILE_DEV, N_CELL * N_TM, 1, MOST, 2))(tile_owner_keys, tile_owner_turns).reshape((NTILES, 1))
    tile_block = plant(jax.random.randint(streams_of[6], (NTILES,), 0, CB_DEV), jax.random.fold_in(streams_of[6], 1), 0, CB_DEV - 1).astype(jnp.int32)
    tile_step = plant(jax.random.randint(streams_of[7], (NTILES,), 0, T_DEV), jax.random.fold_in(streams_of[7], 1), 0, T_DEV - 1).astype(jnp.int32)
    tile_obs = plant(jax.random.randint(streams_of[8], (NTILES,), 0, OBS_DEV), jax.random.fold_in(streams_of[8], 1), 0, OBS_DEV - 1).astype(jnp.int32)
    cell_cov = draw_cell_cov(jax.random.fold_in(streams_of[11], 71), 0)
    time_cov = draw_time_cov(jax.random.fold_in(streams_of[11], 71), 0)
    return dict(solution=solution, residual=residual, direction=direction, noise_var=noise_var, footprints=footprints, tile_owner=tile_owner, tile_block=tile_block, tile_step=tile_step, tile_obs=tile_obs, cell_cov=cell_cov, time_cov=time_cov)


def reference(solution, residual, direction, noise_var, footprints, tile_owner, tile_block, tile_step, tile_obs, cell_cov, time_cov):
    cell_local = NC // N_CELL
    time_local = NT // N_TM
    block_local = cell_local // BLK
    owner_dev = tile_owner[:, 0].astype(jnp.int32)
    source_dev = (jnp.arange(NTILES) // TILE_DEV).astype(jnp.int32)
    obs_index = (source_dev * OBS_DEV + tile_obs).astype(jnp.int32)
    dir_tile = direction[obs_index].astype(jnp.bfloat16).astype(jnp.float32)
    global_block = ((owner_dev // N_TM) * block_local + tile_block).astype(jnp.int32)
    global_time = ((owner_dev % N_TM) * time_local + tile_step).astype(jnp.int32)
    tile_values = footprints.astype(jnp.float32)
    flux_time = jnp.zeros((NT, NC // BLK, BLK), jnp.float32)
    flux_time = flux_time.at[global_time, global_block].add(dir_tile[:, None] * tile_values)
    flux_grid = flux_time.reshape(NT, NC).T.astype(jnp.bfloat16)
    mixed_cells = jnp.dot(cell_cov, flux_grid, preferred_element_type=jnp.float32).astype(jnp.bfloat16)
    smoothed = jnp.dot(mixed_cells, time_cov, preferred_element_type=jnp.float32).astype(jnp.bfloat16)
    columns = smoothed.T.reshape(NT, NC // BLK, BLK)[global_time, global_block].astype(jnp.float32)
    tile_dots = jnp.sum(tile_values * columns, axis=1)
    applied = jax.ops.segment_sum(tile_dots, obs_index, num_segments=NOBS) + noise_var * direction
    norm_now = jnp.sum(residual * residual)
    curvature = jnp.sum(direction * applied)
    step_size = norm_now / curvature
    new_solution = solution + step_size * direction
    new_residual = residual - step_size * applied
    norm_next = jnp.sum(new_residual * new_residual)
    new_direction = new_residual + (norm_next / norm_now) * direction
    return (new_solution, new_residual, new_direction)
```

```python
import functools

import jax
import jax.numpy as jnp
from jax import lax
from jax.experimental import pallas as pl
from jax.experimental.pallas import tpu as pltpu
from jax.sharding import PartitionSpec as P

AXES = ("cell", "tm")
LANES = 128
META = 16
UNROLL = 8
COPIES = 4
F32 = jnp.float32
BF16 = jnp.bfloat16
VMEM = pl.BlockSpec(memory_space=pltpu.VMEM)
SMEM = pl.BlockSpec(memory_space=pltpu.SMEM)


def pack_kernel(devices, cap, owner, step, block, obs, dir_col, tiles, send, slot_obs, rhs):
    rows = owner.shape[0]
    obs_local = dir_col.shape[0]
    width = tiles.shape[1]
    groups = devices * cap // LANES
    lane_i = lax.broadcasted_iota(jnp.int32, (LANES, 2 * LANES), 0)
    lane_j = lax.broadcasted_iota(jnp.int32, (LANES, 2 * LANES), 1)
    tri = jnp.where((lane_i <= lane_j) | (lane_j >= LANES), 1.0, 0.0).astype(BF16)
    dev_i = lax.broadcasted_iota(jnp.int32, (devices, LANES), 0)
    obs_i = lax.broadcasted_iota(jnp.int32, (obs_local, LANES), 0)
    eight = lax.broadcasted_iota(jnp.int32, (8, LANES), 0)
    directions = jnp.broadcast_to(dir_col[...], (obs_local, LANES))
    rhs[:, :width] = tiles[...]
    carry = jnp.zeros((devices, LANES), F32)
    slots = []
    for r in range(rows):
        own = owner[r : r + 1, :]
        hot = jnp.where(dev_i == own, 1.0, 0.0)
        counts = jnp.dot(hot.astype(BF16), tri, preferred_element_type=F32)
        rank = jnp.sum(hot * (counts[:, :LANES] + carry), axis=0, keepdims=True)
        carry = carry + counts[:, LANES:]
        slots.append(own * cap + rank.astype(jnp.int32) - 1)
        seen = obs[r : r + 1, :]
        d = jnp.sum(jnp.where(obs_i == seen, directions, 0.0), axis=0, keepdims=True)
        hi = d.astype(BF16).astype(F32)
        mid = (d - hi).astype(BF16).astype(F32)
        low = d - hi - mid
        meta = jnp.zeros((8, LANES), F32)
        fields = (hi, mid, low, step[r : r + 1, :].astype(F32), block[r : r + 1, :].astype(F32), seen.astype(F32) + 1.0)
        for f, value in enumerate(fields):
            meta = jnp.where(eight == f, value, meta)
        full = jnp.concatenate([meta, jnp.zeros((LANES - 8, LANES), F32)], axis=0)
        rhs[r * LANES : (r + 1) * LANES, width:] = full.T.astype(BF16)
    slot_i = lax.broadcasted_iota(jnp.int32, (LANES, LANES), 0)
    share = LANES // cap

    def group(g, _):
        base = slot_i + g * LANES
        pick = jnp.concatenate([jnp.where(base == s, 1.0, 0.0).astype(BF16) for s in slots], axis=1)
        out = jnp.dot(pick, rhs[...], preferred_element_type=F32)
        meta = out[:, width:].T
        for q in range(share):
            send[g * share + q, :cap, :] = out[q * cap : (q + 1) * cap, :width].astype(BF16)
            part = meta[:META, :]
            if q:
                part = jnp.concatenate([part[:, q * cap :], part[:, : q * cap]], axis=1)
            send[g * share + q, cap:, :] = part.astype(BF16)
        slot_obs[pl.ds(g, 1), :] = meta[5:6, :]
        return 0

    lax.fori_loop(0, groups, group, 0)


def scatter_kernel(devices, cap, sizes, time_local, place, weight, count, got, *refs):
    outs, (values, *sums) = refs[: len(sizes)], refs[len(sizes) :]
    for s in sums:
        s[...] = jnp.zeros_like(s)

    def widen(s, _):
        values[pl.ds(s * cap, cap), :] = got[s, :cap, :].astype(F32)
        return 0

    lax.fori_loop(0, devices, widen, 0)

    def source(s, _):
        def some(k, _):
            base = s * cap + k * UNROLL
            for u in range(UNROLL):
                at = place[base + u]
                acc = sums[u % COPIES]
                acc[pl.ds(at, 1), :] += values[pl.ds(base + u, 1), :] * weight[base + u]
            return 0

        return lax.fori_loop(0, pl.cdiv(count[s], UNROLL), some, 0)

    lax.fori_loop(0, devices, source, 0)
    first = 0
    for out, size in zip(outs, sizes):
        for b in range(size):
            rows = slice((first + b) * time_local, (first + b + 1) * time_local)
            total = sums[0][rows, :]
            for s in sums[1:]:
                total = total + s[rows, :]
            out[:, b * LANES : (b + 1) * LANES] = total.astype(BF16)
        first += size


def gather_kernel(devices, cap, block_local, time_local, place, count, got, smoothed, dirs, residual, direction, noise, ret, flat, picked):
    for b in range(block_local):
        part = smoothed[b * LANES : (b + 1) * LANES, :].T
        flat[b * time_local : (b + 1) * time_local, :] = part.astype(BF16).astype(F32)
    picked[...] = jnp.zeros_like(picked)

    def source(s, _):
        def some(k, _):
            base = s * cap + k * UNROLL
            for u in range(UNROLL):
                picked[pl.ds(base + u, 1), :] = flat[pl.ds(place[base + u], 1), :]
            return 0

        return lax.fori_loop(0, pl.cdiv(count[s], UNROLL), some, 0)

    lax.fori_loop(0, devices, source, 0)
    share = LANES // cap

    def dots(g, total):
        tiles = [got[g * share + q, :cap, :].astype(F32) for q in range(share)]
        tiles = tiles[0] if share == 1 else jnp.concatenate(tiles, axis=0)
        prod = tiles * picked[pl.ds(g * LANES, LANES), :]
        row = jnp.sum(prod.T, axis=0, keepdims=True)
        for q in range(share):
            part = row
            if q:
                part = jnp.concatenate([row[:, q * cap :], row[:, : q * cap]], axis=1)
            ret[g * share + q, 0:1, :] = part
        return total + row * dirs[pl.ds(g, 1), :]

    total = lax.fori_loop(0, devices // share, dots, jnp.zeros((1, LANES), F32))
    d = direction[...]
    curv = jnp.sum(total) + jnp.sum(noise[...] * d * d)
    norm = jnp.sum(residual[...] * residual[...])
    lane = lax.broadcasted_iota(jnp.int32, (1, LANES), 1)
    scalars = jnp.where(lane == 0, curv, jnp.where(lane == 1, norm, 0.0))

    def spread(s, _):
        ret[s, 1:2, :] = scalars
        return 0

    lax.fori_loop(0, devices, spread, 0)


def finish_kernel(devices, dots, scalars, slot_obs, solution, residual, direction, noise, new_solution, new_residual, share, ratio):
    rows = slot_obs.shape[0]
    blocks = solution.shape[0]
    obs_local = blocks * LANES
    obs_i = lax.broadcasted_iota(jnp.int32, (obs_local, LANES), 0).astype(F32) + 1.0
    acc = jnp.zeros((obs_local, LANES), F32)
    for r in range(rows):
        acc = acc + jnp.where(obs_i == slot_obs[r : r + 1, :], dots[r : r + 1, :], 0.0)
    parts = [jnp.sum(acc[b * LANES : (b + 1) * LANES, :].T, axis=0, keepdims=True) for b in range(blocks)]
    d = direction[...]
    applied = jnp.concatenate(parts, axis=0) + noise[...] * d
    sums = jnp.sum(scalars[...], axis=0, keepdims=True)
    lane = lax.broadcasted_iota(jnp.int32, (1, LANES), 1)
    curvature = jnp.sum(jnp.where(lane == 0, sums, 0.0), keepdims=True)
    norm_now = jnp.sum(jnp.where(lane == 1, sums, 0.0), keepdims=True)
    step = norm_now / curvature
    new_solution[...] = solution[...] + step * d
    fresh = residual[...] - step * applied
    new_residual[...] = fresh
    share[...] = jnp.broadcast_to(jnp.sum(fresh * fresh, keepdims=True).reshape(1, 1, 1), share.shape)
    ratio[...] = jnp.broadcast_to(norm_now, ratio.shape)


def product_kernel(step, sizes, planes, here, *refs):
    flux, cov, refs = refs[: -2 - (step > 0)], refs[-2 - (step > 0)], refs[-1 - (step > 0) :]
    out = refs[-1]
    q = pl.program_id(1)

    if step:

        @pl.when(q == 0)
        def _():
            out[...] = refs[0][...]

    for side in range(len(flux) // len(sizes)):
        plane = meets(step, side, here[0])

        @pl.when((q == side) & (plane >= 0) & (plane < planes))
        def _(side=side):
            total, at = None, 0
            for k, size in enumerate(sizes):
                part = jnp.dot(cov[:, at : at + size], flux[side * len(sizes) + k][...], preferred_element_type=F32)
                total = part if total is None else total + part
                at += size
            out[...] = out[...] + total if step else total


def meets(step, side, here):
    return here + step if side else here - step


def product(step, sides, cell_cov, acc, planes, here):
    flux = [x for side in sides for x in side]
    sizes = [x.shape[0] for x in sides[0]]
    width, steps = sum(sizes), flux[0].shape[1]
    out = cell_cov.shape[0]
    tile = next(t for t in (384, 256, 128) if out % t == 0)
    keep = pl.BlockSpec((tile, steps), lambda i, q, h: (i, 0))

    def column(i, q, h):
        left = h[0] - step
        right = h[0] + step
        first = jnp.where(left >= 0, left, jnp.minimum(right, planes - 1))
        second = jnp.where(right < planes, right, jnp.maximum(left, 0))
        return i, jnp.where(q == 0, first, second)

    return pl.pallas_call(
        functools.partial(product_kernel, step, sizes, planes),
        grid_spec=pltpu.PrefetchScalarGridSpec(
            num_scalar_prefetch=1,
            grid=(out // tile, len(sides)),
            in_specs=[pl.BlockSpec(x.shape, lambda i, q, h: (0, 0)) for x in flux]
            + [pl.BlockSpec((tile, width), column)] + ([keep] if step else []),
            out_specs=keep,
        ),
        out_shape=jax.ShapeDtypeStruct((out, steps), F32),
        cost_estimate=pl.CostEstimate(flops=2 * steps * width * out, bytes_accessed=2 * out * width, transcendentals=0),
        name="product",
    )(here, *flux, cell_cov, *([acc] if step else []))


def shift(x, by):
    n = lax.axis_size("cell")
    return lax.ppermute(x, "cell", [(i, i + by) for i in range(n) if 0 <= i + by < n])


def smooth(flux, cell_cov, time_cov):
    n = lax.axis_size("cell")
    here = lax.axis_index("cell").astype(jnp.int32).reshape(1)
    mixed = []
    for f in flux:
        whole = lax.all_gather(f, "tm", axis=0, tiled=True)
        part = lax.dot_general(whole, time_cov, (((0,), (1,)), ((), ())), preferred_element_type=F32)
        mixed.append(part.astype(BF16))
    right, left = mixed, mixed
    total = product(0, [mixed], cell_cov, None, n, here)
    for s in range(1, n):
        right = [shift(x, 1) for x in right]
        left = [shift(x, -1) for x in left]
        total = product(s, [right, left], cell_cov, total, n, here)
    return total


def local(solution, residual, direction, noise_var, footprints, tile_owner, tile_block, tile_step, tile_obs, cell_cov, time_cov):
    devices = lax.axis_size("cell") * lax.axis_size("tm")
    tile_count, block_len = footprints.shape
    cell_local = cell_cov.shape[0]
    time_local = time_cov.shape[0]
    block_local = cell_local // block_len
    obs_local = direction.shape[0]
    cap = max(2, 2 * tile_count // devices)
    slots = devices * cap
    assert block_len == LANES and LANES % cap == 0 and cap % UNROLL == 0
    assert max(time_local, block_local, obs_local) <= 256
    half = (block_local + 1) // 2
    sizes = (half, block_local - half)
    rows = (tile_count // LANES, LANES)
    send, slot_obs = pl.pallas_call(
        functools.partial(pack_kernel, devices, cap),
        out_shape=(
            jax.ShapeDtypeStruct((devices, cap + META, LANES), BF16),
            jax.ShapeDtypeStruct((slots // LANES, LANES), F32),
        ),
        in_specs=[VMEM] * 6,
        out_specs=(VMEM, VMEM),
        scratch_shapes=[pltpu.VMEM((tile_count, 2 * LANES), BF16)],
        name="pack",
    )(
        tile_owner.reshape(rows),
        tile_step.reshape(rows),
        tile_block.reshape(rows),
        tile_obs.reshape(rows),
        direction.reshape(obs_local, 1),
        footprints,
    )
    got = lax.all_to_all(send, AXES, split_axis=0, concat_axis=0, tiled=True)
    meta = got[:, cap : cap + 6, :cap].astype(F32)
    place = (meta[:, 4] * time_local + meta[:, 3]).astype(jnp.int32).reshape(slots)
    weight = meta[:, 0].reshape(slots)
    dirs = (meta[:, 0] + meta[:, 1] + meta[:, 2]).reshape(slots // LANES, LANES)
    count = jnp.sum((meta[:, 5] > 0).astype(jnp.int32), axis=1)
    flat = pltpu.VMEM((block_local * time_local, LANES), F32)
    flux = pl.pallas_call(
        functools.partial(scatter_kernel, devices, cap, sizes, time_local),
        out_shape=[jax.ShapeDtypeStruct((time_local, size * LANES), BF16) for size in sizes],
        in_specs=[SMEM] * 3 + [VMEM],
        out_specs=[VMEM] * len(sizes),
        scratch_shapes=[pltpu.VMEM((slots, LANES), F32)] + [flat] * COPIES,
        name="scatter",
    )(place, weight, count, got)
    smoothed = smooth(flux, cell_cov, time_cov)
    wide = (obs_local // LANES, LANES)
    solution, residual, direction, noise_var = (x.reshape(wide) for x in (solution, residual, direction, noise_var))
    ret = pl.pallas_call(
        functools.partial(gather_kernel, devices, cap, block_local, time_local),
        out_shape=jax.ShapeDtypeStruct((devices, 2, LANES), F32),
        in_specs=[SMEM] * 2 + [VMEM] * 6,
        out_specs=VMEM,
        scratch_shapes=[flat, pltpu.VMEM((slots, LANES), F32)],
        name="gather",
    )(place, count, got, smoothed, dirs, residual, direction, noise_var)
    back = lax.all_to_all(ret, AXES, split_axis=0, concat_axis=0, tiled=True)
    new_solution, new_residual, share, norm_now = pl.pallas_call(
        functools.partial(finish_kernel, devices),
        out_shape=(
            jax.ShapeDtypeStruct(wide, F32),
            jax.ShapeDtypeStruct(wide, F32),
            jax.ShapeDtypeStruct((devices, 1, LANES), F32),
            jax.ShapeDtypeStruct((1, LANES), F32),
        ),
        in_specs=[VMEM] * 7,
        out_specs=(VMEM,) * 4,
        name="finish",
    )(back[:, 0, :cap].reshape(slots // LANES, LANES), back[:, 1, :], slot_obs, solution, residual, direction, noise_var)
    shares = lax.all_to_all(share, AXES, split_axis=0, concat_axis=0, tiled=True)
    norm_next = jnp.sum(shares[:, 0, 0])
    new_direction = new_residual + norm_next / norm_now[0, 0] * direction
    return tuple(x.reshape(obs_local) for x in (new_solution, new_residual, new_direction))


def solution(mesh):
    shared = P(AXES)
    return jax.shard_map(
        local,
        mesh=mesh,
        in_specs=(shared,) * 4 + (P(AXES, None), P(AXES, None)) + (shared,) * 3 + (P("cell", None), P("tm", None)),
        out_specs=(shared,) * 3,
        check_vma=False,
    )
```

```python
import functools

import jax
import jax.numpy as jnp
from jax import lax
from jax.experimental import pallas as pl
from jax.experimental.pallas import tpu as pltpu
from jax.sharding import PartitionSpec as P

AXES = ("cell", "tm")
LANES = 128
META = 16
UNROLL = 8
COPIES = 4
F32 = jnp.float32
BF16 = jnp.bfloat16
VMEM = pl.BlockSpec(memory_space=pltpu.VMEM)
SMEM = pl.BlockSpec(memory_space=pltpu.SMEM)


def pack_kernel(devices, cap, owner, step, block, obs, dir_col, tiles, send, slot_obs, rhs):
    rows = owner.shape[0]
    obs_local = dir_col.shape[0]
    width = tiles.shape[1]
    groups = devices * cap // LANES
    lane_i = lax.broadcasted_iota(jnp.int32, (LANES, 2 * LANES), 0)
    lane_j = lax.broadcasted_iota(jnp.int32, (LANES, 2 * LANES), 1)
    tri = jnp.where((lane_i <= lane_j) | (lane_j >= LANES), 1.0, 0.0).astype(BF16)
    dev_i = lax.broadcasted_iota(jnp.int32, (devices, LANES), 0)
    obs_i = lax.broadcasted_iota(jnp.int32, (obs_local, LANES), 0)
    eight = lax.broadcasted_iota(jnp.int32, (8, LANES), 0)
    directions = jnp.broadcast_to(dir_col[...], (obs_local, LANES))
    rhs[:, :width] = tiles[...]
    carry = jnp.zeros((devices, LANES), F32)
    slots = []
    for r in range(rows):
        own = owner[r : r + 1, :]
        hot = jnp.where(dev_i == own, 1.0, 0.0)
        counts = jnp.dot(hot.astype(BF16), tri, preferred_element_type=F32)
        rank = jnp.sum(hot * (counts[:, :LANES] + carry), axis=0, keepdims=True)
        carry = carry + counts[:, LANES:]
        slots.append(own * cap + rank.astype(jnp.int32) - 1)
        seen = obs[r : r + 1, :]
        d = jnp.sum(jnp.where(obs_i == seen, directions, 0.0), axis=0, keepdims=True)
        hi = d.astype(BF16).astype(F32)
        mid = (d - hi).astype(BF16).astype(F32)
        low = d - hi - mid
        meta = jnp.zeros((8, LANES), F32)
        fields = (hi, mid, low, step[r : r + 1, :].astype(F32), block[r : r + 1, :].astype(F32), seen.astype(F32) + 1.0)
        for f, value in enumerate(fields):
            meta = jnp.where(eight == f, value, meta)
        full = jnp.concatenate([meta, jnp.zeros((LANES - 8, LANES), F32)], axis=0)
        rhs[r * LANES : (r + 1) * LANES, width:] = full.T.astype(BF16)
    slot_i = lax.broadcasted_iota(jnp.int32, (LANES, LANES), 0)
    share = LANES // cap

    def group(g, _):
        base = slot_i + g * LANES
        pick = jnp.concatenate([jnp.where(base == s, 1.0, 0.0).astype(BF16) for s in slots], axis=1)
        out = jnp.dot(pick, rhs[...], preferred_element_type=F32)
        meta = out[:, width:].T
        for q in range(share):
            send[g * share + q, :cap, :] = out[q * cap : (q + 1) * cap, :width].astype(BF16)
            part = meta[:META, :]
            if q:
                part = jnp.concatenate([part[:, q * cap :], part[:, : q * cap]], axis=1)
            send[g * share + q, cap:, :] = part.astype(BF16)
        slot_obs[pl.ds(g, 1), :] = meta[5:6, :]
        return 0

    lax.fori_loop(0, groups, group, 0)


def scatter_kernel(devices, cap, sizes, time_local, place, weight, count, got, *refs):
    outs, (values, *sums) = refs[: len(sizes)], refs[len(sizes) :]
    for s in sums:
        s[...] = jnp.zeros_like(s)

    def widen(s, _):
        values[pl.ds(s * cap, cap), :] = got[s, :cap, :].astype(F32)
        return 0

    lax.fori_loop(0, devices, widen, 0)

    def source(s, _):
        def some(k, _):
            base = s * cap + k * UNROLL
            for u in range(UNROLL):
                at = place[base + u]
                acc = sums[u % COPIES]
                acc[pl.ds(at, 1), :] += values[pl.ds(base + u, 1), :] * weight[base + u]
            return 0

        return lax.fori_loop(0, pl.cdiv(count[s], UNROLL), some, 0)

    lax.fori_loop(0, devices, source, 0)
    first = 0
    for out, size in zip(outs, sizes):
        for b in range(size):
            rows = slice((first + b) * time_local, (first + b + 1) * time_local)
            total = sums[0][rows, :]
            for s in sums[1:]:
                total = total + s[rows, :]
            out[:, b * LANES : (b + 1) * LANES] = total.astype(BF16)
        first += size


def gather_kernel(devices, cap, block_local, time_local, place, count, got, smoothed, dirs, residual, direction, noise, ret, flat, picked):
    for b in range(block_local):
        part = smoothed[b * LANES : (b + 1) * LANES, :].T
        flat[b * time_local : (b + 1) * time_local, :] = part.astype(BF16).astype(F32)
    picked[...] = jnp.zeros_like(picked)

    def source(s, _):
        def some(k, _):
            base = s * cap + k * UNROLL
            for u in range(UNROLL):
                picked[pl.ds(base + u, 1), :] = flat[pl.ds(place[base + u], 1), :]
            return 0

        return lax.fori_loop(0, pl.cdiv(count[s], UNROLL), some, 0)

    lax.fori_loop(0, devices, source, 0)
    share = LANES // cap

    def dots(g, total):
        tiles = [got[g * share + q, :cap, :].astype(F32) for q in range(share)]
        tiles = tiles[0] if share == 1 else jnp.concatenate(tiles, axis=0)
        prod = tiles * picked[pl.ds(g * LANES, LANES), :]
        row = jnp.sum(prod.T, axis=0, keepdims=True)
        for q in range(share):
            part = row
            if q:
                part = jnp.concatenate([row[:, q * cap :], row[:, : q * cap]], axis=1)
            ret[g * share + q, 0:1, :] = part
        return total + row * dirs[pl.ds(g, 1), :]

    total = lax.fori_loop(0, devices // share, dots, jnp.zeros((1, LANES), F32))
    d = direction[...]
    curv = jnp.sum(total) + jnp.sum(noise[...] * d * d)
    norm = jnp.sum(residual[...] * residual[...])
    lane = lax.broadcasted_iota(jnp.int32, (1, LANES), 1)
    scalars = jnp.where(lane == 0, curv, jnp.where(lane == 1, norm, 0.0))

    def spread(s, _):
        ret[s, 1:2, :] = scalars
        return 0

    lax.fori_loop(0, devices, spread, 0)


def finish_kernel(devices, dots, scalars, slot_obs, solution, residual, direction, noise, new_solution, new_residual, share, ratio):
    rows = slot_obs.shape[0]
    blocks = solution.shape[0]
    obs_local = blocks * LANES
    obs_i = lax.broadcasted_iota(jnp.int32, (obs_local, LANES), 0).astype(F32) + 1.0
    acc = jnp.zeros((obs_local, LANES), F32)
    for r in range(rows):
        acc = acc + jnp.where(obs_i == slot_obs[r : r + 1, :], dots[r : r + 1, :], 0.0)
    parts = [jnp.sum(acc[b * LANES : (b + 1) * LANES, :].T, axis=0, keepdims=True) for b in range(blocks)]
    d = direction[...]
    applied = jnp.concatenate(parts, axis=0) + noise[...] * d
    sums = jnp.sum(scalars[...], axis=0, keepdims=True)
    lane = lax.broadcasted_iota(jnp.int32, (1, LANES), 1)
    curvature = jnp.sum(jnp.where(lane == 0, sums, 0.0), keepdims=True)
    norm_now = jnp.sum(jnp.where(lane == 1, sums, 0.0), keepdims=True)
    step = norm_now / curvature
    new_solution[...] = solution[...] + step * d
    fresh = residual[...] - step * applied
    new_residual[...] = fresh
    share[...] = jnp.broadcast_to(jnp.sum(fresh * fresh, keepdims=True).reshape(1, 1, 1), share.shape)
    ratio[...] = jnp.broadcast_to(norm_now, ratio.shape)


def product_kernel(step, sizes, planes, here, *refs):
    flux, cov, refs = refs[: -2 - (step > 0)], refs[-2 - (step > 0)], refs[-1 - (step > 0) :]
    out = refs[-1]
    q = pl.program_id(1)

    if step:

        @pl.when(q == 0)
        def _():
            out[...] = refs[0][...]

    for side in range(len(flux) // len(sizes)):
        plane = meets(step, side, here[0])

        @pl.when((q == side) & (plane >= 0) & (plane < planes))
        def _(side=side):
            total, at = None, 0
            for k, size in enumerate(sizes):
                part = jnp.dot(cov[:, at : at + size], flux[side * len(sizes) + k][...], preferred_element_type=F32)
                total = part if total is None else total + part
                at += size
            out[...] = out[...] + total if step else total


def meets(step, side, here):
    return here + step if side else here - step


def product(step, sides, cell_cov, acc, planes, here):
    flux = [x for side in sides for x in side]
    sizes = [x.shape[0] for x in sides[0]]
    width, steps = sum(sizes), flux[0].shape[1]
    out = cell_cov.shape[0]
    tile = next(t for t in (384, 256, 128) if out % t == 0)
    keep = pl.BlockSpec((tile, steps), lambda i, q, h: (i, 0))

    def column(i, q, h):
        left = h[0] - step
        right = h[0] + step
        first = jnp.where(left >= 0, left, jnp.minimum(right, planes - 1))
        second = jnp.where(right < planes, right, jnp.maximum(left, 0))
        return i, jnp.where(q == 0, first, second)

    return pl.pallas_call(
        functools.partial(product_kernel, step, sizes, planes),
        grid_spec=pltpu.PrefetchScalarGridSpec(
            num_scalar_prefetch=1,
            grid=(out // tile, len(sides)),
            in_specs=[pl.BlockSpec(x.shape, lambda i, q, h: (0, 0)) for x in flux]
            + [pl.BlockSpec((tile, width), column)] + ([keep] if step else []),
            out_specs=keep,
        ),
        out_shape=jax.ShapeDtypeStruct((out, steps), F32),
        cost_estimate=pl.CostEstimate(flops=2 * steps * width * out, bytes_accessed=2 * out * width, transcendentals=0),
        name="product",
    )(here, *flux, cell_cov, *([acc] if step else []))


def shift(x, by):
    n = lax.axis_size("cell")
    return lax.ppermute(x, "cell", [(i, i + by) for i in range(n) if 0 <= i + by < n])


def swap(x, bit):
    return lax.ppermute(x, "tm", [(i, i ^ bit) for i in range(lax.axis_size("tm"))])


def after(x, y):
    return lax.optimization_barrier((x, y))[0]


def mix_times(flux, orders, time_cov):
    here = lax.axis_index("tm")
    steps = time_cov.shape[0]

    def columns(masks):
        parts = [lax.dynamic_slice_in_dim(time_cov, (here ^ m) * steps, steps, 1) for m in masks]
        return jnp.concatenate(parts, axis=1)

    def times(x, masks):
        return lax.dot_general(x, columns(masks), (((0,), (1,)), ((), ())), preferred_element_type=F32)

    held = list(flux)
    masks = [[0] for _ in flux]
    for stage in range(len(orders[0]) - 1):
        came = [swap(x, order[stage]) for x, order in zip(held, orders)]
        held = [jnp.concatenate(pair, axis=0) for pair in zip(held, came)]
        masks = [m + [k ^ order[stage] for k in m] for m, order in zip(masks, orders)]
    came = [swap(x, order[-1]) for x, order in zip(held, orders)]
    mine = [times(x, m) for x, m in zip(held, masks)]
    theirs = [times(x, [k ^ order[-1] for k in m]) for x, m, order in zip(came, masks, orders)]
    return [(x + y).astype(BF16) for x, y in zip(mine, theirs)]


def smooth(flux, cell_cov, time_cov):
    n = lax.axis_size("cell")
    here = lax.axis_index("cell").astype(jnp.int32).reshape(1)
    bits = [1 << i for i in range((lax.axis_size("tm") - 1).bit_length())]
    assert 1 << len(bits) == lax.axis_size("tm")
    mixed = mix_times(flux, (bits[1:] + bits[:1], bits[:0:-1] + bits[:1]), time_cov)
    right, left = mixed, mixed
    total = product(0, [mixed], cell_cov, None, n, here)
    for s in range(1, n):
        right = [shift(x, 1) for x in right]
        left = [shift(x, -1) for x in left]
        if s < n - 1:
            held = total
            total = product(s, [right, left], cell_cov, total, n, here)
            right, left = after((right, left), held)
        else:
            total = product(s, [right, left], cell_cov, total, n, here)
    return total


def local(solution, residual, direction, noise_var, footprints, tile_owner, tile_block, tile_step, tile_obs, cell_cov, time_cov):
    devices = lax.axis_size("cell") * lax.axis_size("tm")
    tile_count, block_len = footprints.shape
    cell_local = cell_cov.shape[0]
    time_local = time_cov.shape[0]
    block_local = cell_local // block_len
    obs_local = direction.shape[0]
    cap = max(2, 2 * tile_count // devices)
    slots = devices * cap
    assert block_len == LANES and LANES % cap == 0 and cap % UNROLL == 0
    assert max(time_local, block_local, obs_local) <= 256
    half = (block_local + 1) // 2
    sizes = (half, block_local - half)
    rows = (tile_count // LANES, LANES)
    send, slot_obs = pl.pallas_call(
        functools.partial(pack_kernel, devices, cap),
        out_shape=(
            jax.ShapeDtypeStruct((devices, cap + META, LANES), BF16),
            jax.ShapeDtypeStruct((slots // LANES, LANES), F32),
        ),
        in_specs=[VMEM] * 6,
        out_specs=(VMEM, VMEM),
        scratch_shapes=[pltpu.VMEM((tile_count, 2 * LANES), BF16)],
        name="pack",
    )(
        tile_owner.reshape(rows),
        tile_step.reshape(rows),
        tile_block.reshape(rows),
        tile_obs.reshape(rows),
        direction.reshape(obs_local, 1),
        footprints,
    )
    got = lax.all_to_all(send, AXES, split_axis=0, concat_axis=0, tiled=True)
    meta = got[:, cap : cap + 6, :cap].astype(F32)
    place = (meta[:, 4] * time_local + meta[:, 3]).astype(jnp.int32).reshape(slots)
    weight = meta[:, 0].reshape(slots)
    dirs = (meta[:, 0] + meta[:, 1] + meta[:, 2]).reshape(slots // LANES, LANES)
    count = jnp.sum((meta[:, 5] > 0).astype(jnp.int32), axis=1)
    flat = pltpu.VMEM((block_local * time_local, LANES), F32)
    flux = pl.pallas_call(
        functools.partial(scatter_kernel, devices, cap, sizes, time_local),
        out_shape=[jax.ShapeDtypeStruct((time_local, size * LANES), BF16) for size in sizes],
        in_specs=[SMEM] * 3 + [VMEM],
        out_specs=[VMEM] * len(sizes),
        scratch_shapes=[pltpu.VMEM((slots, LANES), F32)] + [flat] * COPIES,
        name="scatter",
    )(place, weight, count, got)
    smoothed = smooth(flux, cell_cov, time_cov)
    wide = (obs_local // LANES, LANES)
    solution, residual, direction, noise_var = (x.reshape(wide) for x in (solution, residual, direction, noise_var))
    ret = pl.pallas_call(
        functools.partial(gather_kernel, devices, cap, block_local, time_local),
        out_shape=jax.ShapeDtypeStruct((devices, 2, LANES), F32),
        in_specs=[SMEM] * 2 + [VMEM] * 6,
        out_specs=VMEM,
        scratch_shapes=[flat, pltpu.VMEM((slots, LANES), F32)],
        name="gather",
    )(place, count, got, smoothed, dirs, residual, direction, noise_var)
    back = lax.all_to_all(ret, AXES, split_axis=0, concat_axis=0, tiled=True)
    new_solution, new_residual, share, norm_now = pl.pallas_call(
        functools.partial(finish_kernel, devices),
        out_shape=(
            jax.ShapeDtypeStruct(wide, F32),
            jax.ShapeDtypeStruct(wide, F32),
            jax.ShapeDtypeStruct((devices, 1, LANES), F32),
            jax.ShapeDtypeStruct((1, LANES), F32),
        ),
        in_specs=[VMEM] * 7,
        out_specs=(VMEM,) * 4,
        name="finish",
    )(back[:, 0, :cap].reshape(slots // LANES, LANES), back[:, 1, :], slot_obs, solution, residual, direction, noise_var)
    shares = lax.all_to_all(share, AXES, split_axis=0, concat_axis=0, tiled=True)
    norm_next = jnp.sum(shares[:, 0, 0])
    new_direction = new_residual + norm_next / norm_now[0, 0] * direction
    return tuple(x.reshape(obs_local) for x in (new_solution, new_residual, new_direction))


def solution(mesh):
    shared = P(AXES)
    return jax.shard_map(
        local,
        mesh=mesh,
        in_specs=(shared,) * 4 + (P(AXES, None), P(AXES, None)) + (shared,) * 3 + (P("cell", None), P("tm", None)),
        out_specs=(shared,) * 3,
        check_vma=False,
    )
```

```python
import functools
import math

import jax
import jax.numpy as jnp
from jax import lax
from jax.experimental import pallas as pl
from jax.experimental.pallas import tpu as pltpu
from jax.sharding import PartitionSpec as P


AXES = ("cell", "tm")
LANES = 128
META = 16
GRANT = 24 << 20
LAG = 2.5
UNROLL = 8
COPIES = 4
F32 = jnp.float32
BF16 = jnp.bfloat16
VMEM = pl.BlockSpec(memory_space=pltpu.VMEM)
SMEM = pl.BlockSpec(memory_space=pltpu.SMEM)


def pack_kernel(devices, cap, owner, step, block, obs, directions, tiles, send, slot_obs, rhs, pick):
    rows = owner.shape[0]
    obs_local = directions.shape[0] * LANES
    width = tiles.shape[1]
    groups = devices * cap // LANES
    lane_i = lax.broadcasted_iota(jnp.int32, (LANES, 2 * LANES), 0)
    lane_j = lax.broadcasted_iota(jnp.int32, (LANES, 2 * LANES), 1)
    tri = jnp.where((lane_i <= lane_j) | (lane_j >= LANES), 1.0, 0.0).astype(BF16)
    dev_i = lax.broadcasted_iota(jnp.int32, (devices, LANES), 0)
    obs_i = lax.broadcasted_iota(jnp.int32, (obs_local, LANES), 0)
    eight = lax.broadcasted_iota(jnp.int32, (8, LANES), 0)
    spread = [jnp.broadcast_to(directions[b : b + 1, :], (LANES, LANES)).T for b in range(obs_local // LANES)]
    spread = jnp.concatenate(spread, axis=0)
    rhs[:, :width] = tiles[...]
    carry = jnp.zeros((devices, LANES), F32)
    slots = []
    for r in range(rows):
        own = owner[r : r + 1, :]
        hot = jnp.where(dev_i == own, 1.0, 0.0)
        counts = jnp.dot(hot.astype(BF16), tri, preferred_element_type=F32)
        rank = jnp.sum(hot * (counts[:, :LANES] + carry), axis=0, keepdims=True)
        carry = carry + counts[:, LANES:]
        slots.append(own * cap + rank.astype(jnp.int32) - 1)
        seen = obs[r : r + 1, :]
        d = jnp.sum(jnp.where(obs_i == seen, spread, 0.0), axis=0, keepdims=True)
        hi = d.astype(BF16).astype(F32)
        mid = (d - hi).astype(BF16).astype(F32)
        low = d - hi - mid
        meta = jnp.zeros((8, LANES), F32)
        fields = (hi, mid, low, step[r : r + 1, :].astype(F32), block[r : r + 1, :].astype(F32), seen.astype(F32) + 1.0)
        for f, value in enumerate(fields):
            meta = jnp.where(eight == f, value, meta)
        full = jnp.concatenate([meta, jnp.zeros((LANES - 8, LANES), F32)], axis=0)
        rhs[r * LANES : (r + 1) * LANES, width:] = full.T.astype(BF16)
    slot_i = lax.broadcasted_iota(jnp.int32, (LANES, LANES), 0).astype(F32).astype(BF16)
    one, zero = jnp.ones((LANES, LANES), BF16), jnp.zeros((LANES, LANES), BF16)
    share = LANES // cap
    batch = math.gcd(groups, 4)

    def some(i, _):
        for u in range(batch):
            base = (i * batch + u) * LANES
            for r, slot in enumerate(slots):
                near = jnp.clip(slot - base, -1, LANES).astype(F32).astype(BF16)
                near = jnp.broadcast_to(near, (LANES, LANES))
                pick[u * LANES : (u + 1) * LANES, r * LANES : (r + 1) * LANES] = jnp.where(slot_i == near, one, zero)
        out = jnp.dot(pick[...], rhs[...], preferred_element_type=F32)
        for u in range(batch):
            g = i * batch + u
            meta = out[u * LANES : (u + 1) * LANES, width:].T
            for q in range(share):
                send[g * share + q, :cap, :] = out[u * LANES + q * cap : u * LANES + (q + 1) * cap, :width].astype(BF16)
                part = meta[:META, :]
                if q:
                    part = jnp.concatenate([part[:, q * cap :], part[:, : q * cap]], axis=1)
                send[g * share + q, cap:, :] = part.astype(BF16)
            slot_obs[pl.ds(g, 1), :] = meta[5:6, :]
        return 0

    lax.fori_loop(0, groups // batch, some, 0)


def scatter_kernel(devices, cap, sizes, time_local, place, weight, count, got, *refs):
    outs, (values, *sums) = refs[: len(sizes)], refs[len(sizes) :]
    for s in sums:
        s[...] = jnp.zeros_like(s)

    def widen(s, _):
        values[pl.ds(s * cap, cap), :] = got[s, :cap, :].astype(F32)
        return 0

    lax.fori_loop(0, devices, widen, 0)

    def source(s, _):
        def some(k, _):
            base = s * cap + k * UNROLL
            for u in range(UNROLL):
                at = place[base + u]
                acc = sums[u % COPIES]
                acc[pl.ds(at, 1), :] += values[pl.ds(base + u, 1), :] * weight[base + u]
            return 0

        return lax.fori_loop(0, pl.cdiv(count[s], UNROLL), some, 0)

    lax.fori_loop(0, devices, source, 0)
    first = 0
    for out, size in zip(outs, sizes):
        for b in range(size):
            rows = slice((first + b) * time_local, (first + b + 1) * time_local)
            total = sums[0][rows, :]
            for s in sums[1:]:
                total = total + s[rows, :]
            out[:, b * LANES : (b + 1) * LANES] = total.astype(BF16)
        first += size


def gather_kernel(devices, cap, block_local, time_local, place, count, got, smoothed, dirs, residual, direction, noise, ret, flat, picked):
    for b in range(block_local):
        part = smoothed[b * LANES : (b + 1) * LANES, :].T
        flat[b * time_local : (b + 1) * time_local, :] = part.astype(BF16).astype(F32)
    picked[...] = jnp.zeros_like(picked)

    def source(s, _):
        def some(k, _):
            base = s * cap + k * UNROLL
            for u in range(UNROLL):
                picked[pl.ds(base + u, 1), :] = flat[pl.ds(place[base + u], 1), :]
            return 0

        return lax.fori_loop(0, pl.cdiv(count[s], UNROLL), some, 0)

    lax.fori_loop(0, devices, source, 0)
    share = LANES // cap

    def dots(g, total):
        tiles = [got[g * share + q, :cap, :].astype(F32) for q in range(share)]
        tiles = tiles[0] if share == 1 else jnp.concatenate(tiles, axis=0)
        prod = tiles * picked[pl.ds(g * LANES, LANES), :]
        row = jnp.sum(prod.T, axis=0, keepdims=True)
        for q in range(share):
            part = row
            if q:
                part = jnp.concatenate([row[:, q * cap :], row[:, : q * cap]], axis=1)
            ret[g * share + q, 0:1, :] = part
        return total + row * dirs[pl.ds(g, 1), :]

    total = lax.fori_loop(0, devices // share, dots, jnp.zeros((1, LANES), F32))
    d = direction[...]
    curv = jnp.sum(total) + jnp.sum(noise[...] * d * d)
    norm = jnp.sum(residual[...] * residual[...])
    lane = lax.broadcasted_iota(jnp.int32, (1, LANES), 1)
    scalars = jnp.where(lane == 0, curv, jnp.where(lane == 1, norm, 0.0))

    def spread(s, _):
        ret[s, 1:2, :] = scalars
        return 0

    lax.fori_loop(0, devices, spread, 0)


def finish_kernel(devices, cap, back, slot_obs, solution, residual, direction, noise, new_solution, new_residual, share, ratio):
    rows = slot_obs.shape[0]
    blocks = solution.shape[0]
    obs_local = blocks * LANES
    obs_i = lax.broadcasted_iota(jnp.int32, (obs_local, LANES), 0).astype(F32) + 1.0
    acc = jnp.zeros((obs_local, LANES), F32)
    per = LANES // cap
    for r in range(rows):
        dots = [back[r * per + q, 0:1, :cap] for q in range(per)]
        dots = dots[0] if per == 1 else jnp.concatenate(dots, axis=1)
        acc = acc + jnp.where(obs_i == slot_obs[r : r + 1, :], dots, 0.0)
    parts = [jnp.sum(acc[b * LANES : (b + 1) * LANES, :].T, axis=0, keepdims=True) for b in range(blocks)]
    d = direction[...]
    applied = jnp.concatenate(parts, axis=0) + noise[...] * d
    sums = back[0, 1:2, :]
    for s in range(1, devices):
        sums = sums + back[s, 1:2, :]
    lane = lax.broadcasted_iota(jnp.int32, (1, LANES), 1)
    curvature = jnp.sum(jnp.where(lane == 0, sums, 0.0), keepdims=True)
    norm_now = jnp.sum(jnp.where(lane == 1, sums, 0.0), keepdims=True)
    step = norm_now / curvature
    new_solution[...] = solution[...] + step * d
    fresh = residual[...] - step * applied
    new_residual[...] = fresh
    share[...] = jnp.broadcast_to(jnp.sum(fresh * fresh, keepdims=True).reshape(1, 1, 1), share.shape)
    ratio[...] = jnp.broadcast_to(norm_now, ratio.shape)


def turn_kernel(devices, shares, norm_now, fresh, direction, new_direction):
    total = shares[0]
    for s in range(1, devices):
        total = total + shares[s]
    new_direction[...] = fresh[...] + total / norm_now[...] * direction[...]


def product_kernel(step, first, count, parts, plan, *refs):
    flux, cov, refs = refs[:count], refs[count : count + parts], refs[count + parts :]
    held, out = refs[-1], refs[-2]

    @pl.when(pl.program_id(0) == 0)
    def _():
        for c in range(count):

            @pl.when(plan[step, 0] == c)
            def _(c=c):
                held[...] = flux[c][...]

    unit = cov[0].shape[1]
    total = None if first else refs[0][...]
    for k in range(parts):
        part = jnp.dot(cov[k][...], held[k * unit : (k + 1) * unit, :], preferred_element_type=F32)
        total = part if total is None else total + part
    out[...] = total


def turns(planes):
    out = [[(0, 0)]]
    for s in range(1, planes):
        out.append([(k, side) for k in [s] + [s - m for m in range(planes // 2, s)] for side in (0, 1)])
    return out


def plan_of(planes, here):
    longer = jnp.where(here >= planes - 1 - here, 0, 1)
    most = jnp.maximum(here, planes - 1 - here)
    rows = []
    for s, listed in enumerate(turns(planes)):
        late = s > most
        k = jnp.where(late, s - most, s)
        side = jnp.where(late, 1 - longer, longer)
        which = jnp.zeros_like(here)
        for c, (at, where) in enumerate(listed):
            which = jnp.where((k == at) & (side == where), c, which)
        rows.append(jnp.stack([which, here + jnp.where(side == 1, k, -k)]))
    return jnp.stack(rows).astype(jnp.int32)


def product(step, flux, at, whole, cell_cov, acc, plan):
    size, steps = flux[0].shape
    unit = math.gcd(size, at, whole)
    parts = size // unit
    out = cell_cov.shape[0]
    tile = next(t for t in (768, 384, 256, 128) if out % t == 0)
    keep = pl.BlockSpec((tile, steps), lambda i, p: (i, 0))

    def column(k, i, p):
        return i, p[step, 1] * (whole // unit) + at // unit + k

    return pl.pallas_call(
        functools.partial(product_kernel, step, acc is None, len(flux), parts),
        grid_spec=pltpu.PrefetchScalarGridSpec(
            num_scalar_prefetch=1,
            grid=(out // tile,),
            in_specs=[pl.BlockSpec(x.shape, lambda i, p: (0, 0)) for x in flux]
            + [pl.BlockSpec((tile, unit), functools.partial(column, k)) for k in range(parts)]
            + ([] if acc is None else [keep]),
            out_specs=keep,
            scratch_shapes=[pltpu.VMEM((size, steps), BF16)],
        ),
        out_shape=jax.ShapeDtypeStruct((out, steps), F32),
        compiler_params=pltpu.CompilerParams(vmem_limit_bytes=GRANT),
        cost_estimate=pl.CostEstimate(flops=2 * steps * size * out, bytes_accessed=2 * out * size, transcendentals=0),
        name="product",
    )(plan, *flux, *[cell_cov] * parts, *([] if acc is None else [acc]))


def shift(x, by):
    n = lax.axis_size("cell")
    return lax.ppermute(x, "cell", [(i, i + by) for i in range(n) if 0 <= i + by < n])


def swap(x, bit):
    return lax.ppermute(x, "tm", [(i, i ^ bit) for i in range(lax.axis_size("tm"))])


def after(x, y):
    return lax.optimization_barrier((x, y))[0]


def mix_times(flux, orders, time_cov):
    here = lax.axis_index("tm")
    steps = time_cov.shape[0]

    def columns(masks):
        parts = [lax.dynamic_slice_in_dim(time_cov, (here ^ m) * steps, steps, 1) for m in masks]
        return jnp.concatenate(parts, axis=1)

    def times(x, masks):
        return lax.dot_general(x, columns(masks), (((0,), (1,)), ((), ())), preferred_element_type=F32)

    pairs = [flux[k : k + 2] for k in range(0, len(flux), 2)]
    out = []
    for pair in pairs:
        held, masks = pair, [[0], [0]]
        if out:
            held = [after(x, out[-1]) for x in held]
        for stage in range(len(orders[0]) - 1):
            came = [swap(x, order[stage]) for x, order in zip(held, orders)]
            held = [jnp.concatenate(both, axis=0) for both in zip(held, came)]
            masks = [m + [k ^ order[stage] for k in m] for m, order in zip(masks, orders)]
        came = [swap(x, order[-1]) for x, order in zip(held, orders)]
        mine = [times(x, m) for x, m in zip(held, masks)]
        theirs = [times(x, [k ^ order[-1] for k in m]) for x, m, order in zip(came, masks, orders)]
        mixed = jnp.concatenate([(x + y).astype(BF16) for x, y in zip(mine, theirs)], axis=0)
        out.append(mixed)
    return out


def smooth(flux, cell_cov, time_cov):
    n = lax.axis_size("cell")
    plan = plan_of(n, lax.axis_index("cell"))
    bits = [1 << i for i in range((lax.axis_size("tm") - 1).bit_length())]
    assert 1 << len(bits) == lax.axis_size("tm")
    chunks = mix_times(flux, (bits[1:] + bits[:1], bits[:0:-1] + bits[:1]), time_cov)
    whole = cell_cov.shape[0]
    starts = [sum(x.shape[0] for x in chunks[:k]) for k in range(len(chunks))]
    right, left = list(chunks), list(chunks)
    total, done, there = None, {}, {}
    listed = turns(n)
    for s, k in sorted(((s, k) for s in range(n) for k in range(len(chunks))), key=lambda x: (x[0] + LAG * x[1], x)):
        if s > 1:
            right[k] = after(right[k], done[s - 2, k])
            left[k] = after(left[k], done[s - 2, k])
        if s:
            right[k] = shift(right[k], 1)
            left[k] = shift(left[k], -1)
        there[k, s, 0], there[k, s, 1] = right[k], left[k]
        flux = [there[k, step, side] for step, side in listed[s]]
        total = done[s, k] = product(s, flux, starts[k], whole, cell_cov, total, plan)
    return total


def local(solution, residual, direction, noise_var, footprints, tile_owner, tile_block, tile_step, tile_obs, cell_cov, time_cov):
    devices = lax.axis_size("cell") * lax.axis_size("tm")
    tile_count, block_len = footprints.shape
    cell_local = cell_cov.shape[0]
    time_local = time_cov.shape[0]
    block_local = cell_local // block_len
    obs_local = direction.shape[0]
    cap = max(2, 2 * tile_count // devices)
    slots = devices * cap
    assert block_len == LANES and LANES % cap == 0 and cap % UNROLL == 0
    assert max(time_local, block_local, obs_local) <= 256
    half = (block_local + 1) // 2
    sizes = tuple(x for part in (half, block_local - half) for x in ((part + 1) // 2, part // 2))
    rows = (tile_count // LANES, LANES)
    send, slot_obs = pl.pallas_call(
        functools.partial(pack_kernel, devices, cap),
        out_shape=(
            jax.ShapeDtypeStruct((devices, cap + META, LANES), BF16),
            jax.ShapeDtypeStruct((slots // LANES, LANES), F32),
        ),
        in_specs=[VMEM] * 6,
        out_specs=(VMEM, VMEM),
        scratch_shapes=[pltpu.VMEM((tile_count, 2 * LANES), BF16), pltpu.VMEM((4 * LANES, tile_count), BF16)],
        name="pack",
    )(
        tile_owner.reshape(rows),
        tile_step.reshape(rows),
        tile_block.reshape(rows),
        tile_obs.reshape(rows),
        direction.reshape(obs_local // LANES, LANES),
        footprints,
    )
    got = lax.all_to_all(send, AXES, split_axis=0, concat_axis=0, tiled=True)
    meta = got[:, cap : cap + 6, :cap].astype(F32)
    place = (meta[:, 4] * time_local + meta[:, 3]).astype(jnp.int32).reshape(slots)
    weight = meta[:, 0].reshape(slots)
    dirs = (meta[:, 0] + meta[:, 1] + meta[:, 2]).reshape(slots // LANES, LANES)
    count = jnp.sum((meta[:, 5] > 0).astype(jnp.int32), axis=1)
    flat = pltpu.VMEM((block_local * time_local, LANES), F32)
    flux = pl.pallas_call(
        functools.partial(scatter_kernel, devices, cap, sizes, time_local),
        out_shape=[jax.ShapeDtypeStruct((time_local, size * LANES), BF16) for size in sizes],
        in_specs=[SMEM] * 3 + [VMEM],
        out_specs=[VMEM] * len(sizes),
        scratch_shapes=[pltpu.VMEM((slots, LANES), F32)] + [flat] * COPIES,
        compiler_params=pltpu.CompilerParams(vmem_limit_bytes=GRANT),
        name="scatter",
    )(place, weight, count, got)
    smoothed = smooth(flux, cell_cov, time_cov)
    wide = (obs_local // LANES, LANES)
    solution, residual, direction, noise_var = (x.reshape(wide) for x in (solution, residual, direction, noise_var))
    ret = pl.pallas_call(
        functools.partial(gather_kernel, devices, cap, block_local, time_local),
        out_shape=jax.ShapeDtypeStruct((devices, 2, LANES), F32),
        in_specs=[SMEM] * 2 + [VMEM] * 6,
        out_specs=VMEM,
        scratch_shapes=[flat, pltpu.VMEM((slots, LANES), F32)],
        compiler_params=pltpu.CompilerParams(vmem_limit_bytes=GRANT),
        name="gather",
    )(place, count, got, smoothed, dirs, residual, direction, noise_var)
    back = lax.all_to_all(ret, AXES, split_axis=0, concat_axis=0, tiled=True)
    new_solution, new_residual, share, norm_now = pl.pallas_call(
        functools.partial(finish_kernel, devices, cap),
        out_shape=(
            jax.ShapeDtypeStruct(wide, F32),
            jax.ShapeDtypeStruct(wide, F32),
            jax.ShapeDtypeStruct((devices, 1, LANES), F32),
            jax.ShapeDtypeStruct((1, LANES), F32),
        ),
        in_specs=[VMEM] * 6,
        out_specs=(VMEM,) * 4,
        compiler_params=pltpu.CompilerParams(vmem_limit_bytes=GRANT),
        name="finish",
    )(back, slot_obs, solution, residual, direction, noise_var)
    shares = lax.all_to_all(share, AXES, split_axis=0, concat_axis=0, tiled=True)
    new_direction = pl.pallas_call(
        functools.partial(turn_kernel, devices),
        out_shape=jax.ShapeDtypeStruct(wide, F32),
        in_specs=[VMEM] * 4,
        out_specs=VMEM,
        compiler_params=pltpu.CompilerParams(vmem_limit_bytes=GRANT),
        name="turn",
    )(shares, norm_now, new_residual, direction)
    return tuple(x.reshape(obs_local) for x in (new_solution, new_residual, new_direction))


def solution(mesh):
    shared = P(AXES)
    return jax.shard_map(
        local,
        mesh=mesh,
        in_specs=(shared,) * 4 + (P(AXES, None), P(AXES, None)) + (shared,) * 3 + (P("cell", None), P("tm", None)),
        out_specs=(shared,) * 3,
        check_vma=False,
    )
```
